16 devices in a mesh: tp: 4 (over z, y), dp: 4 (over x, core).
Axes of the slice: x: 2, y: 2, z: 2, core: 2. Of those that a mesh axis runs over, the one named last changes fastest.
Arguments:
- hidden: bfloat16 [8192, 2048], P('dp')
- labels: int32 [8192], P('dp')
- loss_mask: int32 [8192], P('dp')
- norm_gain: bfloat16 [2048], replicated
- w_out: bfloat16 [2048, 32000], P(None, 'tp')
Outputs:
- output 1: float32 [], replicated
- output 2: bfloat16 [8192, 2048], P('dp')
- output 3: float32 [2048, 32000], P(None, 'tp')
- output 4: float32 [2048], replicated
All inputs are finite; a program needn't handle non-finite values.
Results may differ from the reference program's by a relative error of at most 0.001.
Values sent between devices are 32-bit elements.
A program may use at most 1 GiB of HBM per device.

```python
import math
import jax
import jax.numpy as jnp
from jax import lax

D = 2048
V = 32000
TOKENS_DEV = 2048
DATA_SHARDS = 4
TOKENS = TOKENS_DEV * DATA_SHARDS
NORM_EPS = 1e-5


def setup_inputs(seed: int = 0) -> dict:
    rng_key = jax.random.key(seed)
    k_hid, k_lab, k_dens, k_draw, k_gain, k_wout = jax.random.split(rng_key, 6)
    hidden = jax.random.normal(k_hid, (TOKENS, D), jnp.float32)
    labels = jax.random.randint(k_lab, (TOKENS,), 0, V, dtype=jnp.int32)
    labels = labels.at[0].set(V - 1).at[1].set(0)
    density = jax.random.randint(k_dens, (DATA_SHARDS, 1), 20, 96, dtype=jnp.int32)
    coin_draws = jax.random.randint(k_draw, (DATA_SHARDS, TOKENS_DEV), 0, 100, dtype=jnp.int32)
    loss_mask = (coin_draws < density).astype(jnp.int32).reshape(TOKENS).at[0].set(1)
    norm_gain = 1.0 + 0.3 * jax.random.normal(k_gain, (D,), jnp.float32)
    w_scale = math.sqrt(math.log(V) / D)
    w_out = w_scale * jax.random.normal(k_wout, (D, V), jnp.float32)
    return {"hidden": hidden.astype(jnp.bfloat16), "labels": labels, "loss_mask": loss_mask, "norm_gain": norm_gain.astype(jnp.bfloat16), "w_out": w_out.astype(jnp.bfloat16)}


def reference(hidden, labels, loss_mask, norm_gain, w_out):
    mask_f = loss_mask.astype(jnp.float32)
    mask_total = jnp.sum(mask_f)
    gain_f = norm_gain.astype(jnp.float32)
    vocab_ids = jnp.arange(V, dtype=jnp.int32)

    def block_step(acc_in, row_block):
        loss_acc, dw_acc, dgain_acc = acc_in
        h_block, lab_block, mask_block = row_block
        h_f32 = h_block.astype(jnp.float32)
        r_inv = lax.rsqrt(jnp.mean(h_f32 * h_f32, axis=-1, keepdims=True) + NORM_EPS)
        x_hat = h_f32 * r_inv
        normed = (x_hat * gain_f).astype(jnp.bfloat16)
        logits = jnp.dot(normed, w_out, preferred_element_type=jnp.float32)
        row_max = jnp.max(logits, axis=-1, keepdims=True)
        log_norm = row_max + jnp.log(jnp.sum(jnp.exp(logits - row_max), axis=-1, keepdims=True))
        target = jnp.take_along_axis(logits, lab_block[:, None], axis=1)
        row_weight = mask_block[:, None] / mask_total
        loss_acc = loss_acc + jnp.sum(row_weight * (log_norm - target))
        onehot = (vocab_ids[None, :] == lab_block[:, None]).astype(jnp.float32)
        d_logits = (row_weight * (jnp.exp(logits - log_norm) - onehot)).astype(jnp.bfloat16)
        d_normed = jnp.dot(d_logits, w_out.T, preferred_element_type=jnp.float32)
        dw_acc = dw_acc + jnp.dot(normed.T, d_logits, preferred_element_type=jnp.float32)
        dgain_acc = dgain_acc + jnp.sum(d_normed * x_hat, axis=0)
        d_xhat = d_normed * gain_f
        d_hid = r_inv * (d_xhat - x_hat * jnp.mean(d_xhat * x_hat, axis=-1, keepdims=True))
        return (loss_acc, dw_acc, dgain_acc), d_hid.astype(jnp.bfloat16)

    row_blocks = (hidden.reshape(DATA_SHARDS, TOKENS_DEV, D), labels.reshape(DATA_SHARDS, TOKENS_DEV), mask_f.reshape(DATA_SHARDS, TOKENS_DEV))
    acc_start = (jnp.zeros((), jnp.float32), jnp.zeros((D, V), jnp.float32), jnp.zeros((D,), jnp.float32))
    (loss_total, d_w_out, d_gain), d_hidden = lax.scan(block_step, acc_start, row_blocks)
    return loss_total, d_hidden.reshape(TOKENS, D), d_w_out, d_gain
```

```python
import functools

import jax
import jax.numpy as jnp
from jax import lax
from jax.experimental import pallas as pl
from jax.experimental.pallas import tpu as pltpu
from jax.sharding import PartitionSpec as P


NORM_EPS = 1e-5

F32, BF16 = jnp.float32, jnp.bfloat16
VMEM_LIMIT = 66_000_000


def params():
    return pltpu.CompilerParams(dimension_semantics=("arbitrary",), vmem_limit_bytes=VMEM_LIMIT)


def once(shape, index):
    return pl.BlockSpec(shape, index, pipeline_mode=pl.Buffered(1))


def logits_kernel(half, strip, nt, with_target, *refs):
    *refs, zb = refs
    if with_target:
        yt_ref, w_ref, lab_ref, z_ref, m_ref, s_ref, t_ref = refs
    else:
        yt_ref, w_ref, z_ref, m_ref, s_ref = refs
    rows = yt_ref.shape[0] if nt else yt_ref.shape[1]
    j = pl.program_id(0)

    def stats(buf, lo, base, fresh):
        for c in range(0, rows, strip):
            cs = slice(c, c + strip)
            z = buf[lo:lo + half, cs].reshape(half // 8, 8, strip)
            old = m_ref[:, cs]
            if fresh is not None:
                old = jnp.where(fresh, -jnp.inf, old)
            new = jnp.maximum(old, jnp.max(z, axis=0))
            total = jnp.sum(jnp.exp(z - new), axis=0)
            keep = s_ref[:, cs] * jnp.exp(old - new)
            if fresh is not None:
                keep = jnp.where(fresh, 0.0, keep)
            m_ref[:, cs] = new
            s_ref[:, cs] = keep + total
            if with_target:
                row = lax.broadcasted_iota(jnp.int32, (half // 8, 8, strip), 0) * 8 + lax.broadcasted_iota(jnp.int32, (half // 8, 8, strip), 1)
                at = lab_ref[:, cs] - base
                hit = jnp.sum(jnp.where(row == at, z, 0.0), axis=0)
                seen = t_ref[:, cs]
                if fresh is not None:
                    seen = jnp.where(fresh, 0.0, seen)
                t_ref[:, cs] = seen + hit

    @pl.when(j == 0)
    def _():
        z_ref[:half, :] = lax.dot_general(w_ref[:half, :], yt_ref[...], (((1,), (1 if nt else 0,)), ((), ())), preferred_element_type=F32)

    @pl.when(j > 0)
    def _():
        z_ref[:half, :] = lax.dot_general(w_ref[:half, :], yt_ref[...], (((1,), (1 if nt else 0,)), ((), ())), preferred_element_type=F32)
        stats(zb, 0, (2 * j - 1) * half, None)

    zz = lax.dot_general(w_ref[half:, :], yt_ref[...], (((1,), (1 if nt else 0,)), ((), ())), preferred_element_type=F32)
    z_ref[half:, :] = zz
    zb[...] = zz
    stats(z_ref, 0, 2 * j * half, j == 0)

    @pl.when(j == pl.num_programs(0) - 1)
    def _():
        stats(zb, 0, (2 * j + 1) * half, None)


def logits(yt, wt, lab, half=400, strip=256, nt=False):
    rows, d = yt.shape if nt else yt.shape[::-1]
    cols = wt.shape[0]
    with_target = lab is not None
    fixed = lambda shape: once(shape, lambda j: (0, 0))
    stat = jax.ShapeDtypeStruct((8, rows), F32)
    n_stat = 3 if with_target else 2
    ins = [fixed(yt.shape), pl.BlockSpec((2 * half, d), lambda j: (j, 0))]
    args = [yt, wt]
    if with_target:
        ins.append(fixed((1, rows)))
        args.append(lab)
    return pl.pallas_call(
        functools.partial(logits_kernel, half, strip, nt, with_target),
        grid=(cols // (2 * half),),
        in_specs=ins,
        out_specs=[pl.BlockSpec((2 * half, rows), lambda j: (j, 0))] + [fixed((8, rows))] * n_stat,
        out_shape=[jax.ShapeDtypeStruct((cols, rows), F32)] + [stat] * n_stat,
        scratch_shapes=[pltpu.VMEM((half, rows), F32)],
        compiler_params=params(),
        cost_estimate=pl.CostEstimate(flops=2 * rows * d * cols, bytes_accessed=rows * cols * 4 + d * cols * 2, transcendentals=rows * cols),
        name="logits",
    )(*args)


def grad_of(z, lse, weight, hit):
    p = jnp.exp(z - lse)
    return (weight * jnp.where(hit, p - 1.0, p)).astype(BF16)


def dy_kernel(cols, block, chunk, z_ref, w_ref, lse_ref, wt_ref, lab_ref, g_ref, dy_ref, ga, gb):
    rows = z_ref.shape[1]
    n = rows // chunk
    j = pl.program_id(0)
    steps = pl.cdiv(cols, block)
    last = cols - (steps - 1) * block

    @pl.when(j == 0)
    def _():
        dy_ref[...] = jnp.zeros(dy_ref.shape, F32)

    def compute(width):
        def grad(r, buf):
            cs = slice(r * chunk, (r + 1) * chunk)
            v = lax.broadcasted_iota(jnp.int32, (width, chunk), 0)
            g = grad_of(z_ref[:width, cs], lse_ref[:, cs], wt_ref[:, cs], v == lab_ref[:, cs] - j * block)
            buf[:width, :] = g
            g_ref[:width, cs] = g

        def dot(r, buf):
            dy_ref[r * chunk:(r + 1) * chunk, :] += lax.dot_general(buf[:width, :], w_ref[:width, :], (((0,), (0,)), ((), ())), preferred_element_type=F32)

        bufs = (ga, gb)
        grad(0, ga)
        for r in range(n):
            if r + 1 < n:
                grad(r + 1, bufs[(r + 1) % 2])
            dot(r, bufs[r % 2])

    if last == block:
        compute(block)
    else:
        @pl.when(j < steps - 1)
        def _():
            compute(block)

        @pl.when(j == steps - 1)
        def _():
            compute(last)


def grad_and_dy(zt, wt, lse, weight, lab, block=1024, chunk=512):
    cols, rows = zt.shape
    d = wt.shape[1]
    fixed = lambda shape: once(shape, lambda j: (0, 0))
    return pl.pallas_call(
        functools.partial(dy_kernel, cols, block, chunk),
        grid=(pl.cdiv(cols, block),),
        in_specs=[pl.BlockSpec((block, rows), lambda j: (j, 0)), pl.BlockSpec((block, d), lambda j: (j, 0))] + [fixed((1, rows))] * 3,
        out_specs=[pl.BlockSpec((block, rows), lambda j: (j, 0)), fixed((rows, d))],
        out_shape=[jax.ShapeDtypeStruct((cols, rows), BF16), jax.ShapeDtypeStruct((rows, d), F32)],
        scratch_shapes=[pltpu.VMEM((block, chunk), BF16)] * 2,
        compiler_params=params(),
        cost_estimate=pl.CostEstimate(flops=2 * rows * d * cols, bytes_accessed=rows * cols * 6 + d * cols * 2, transcendentals=rows * cols),
        name="dy",
    )(zt, wt, lse, weight, lab)


def dw_kernel(first, block, has_got, half_rows, core_ref, y0_ref, y1_ref, g0_ref, z1_ref, lse_ref, wt_ref, lab_ref, *refs):
    *refs, g1 = refs
    j = pl.program_id(0)
    which = core_ref[0]
    base = which * half_rows + (first + j) * block
    v = lax.broadcasted_iota(jnp.int32, z1_ref.shape, 0)
    g1[...] = grad_of(z1_ref[...], lse_ref[...], wt_ref[...], v == lab_ref[...] - base)
    acc = jnp.dot(g0_ref[...], y0_ref[...], preferred_element_type=F32)
    if has_got:
        acc += refs[0][...]
    acc += jnp.dot(g1[...], y1_ref[...], preferred_element_type=F32)
    refs[-1][...] = acc


def dw_part(which, y0, y1, g0t, z1t, lse, weight, lab, first, blocks, got=None, block=400):
    rows, d = y0.shape
    cols = g0t.shape[0]
    per_half = cols // 2 // block
    fixed = lambda shape: once(shape, lambda j, c: (0, 0))
    part = pl.BlockSpec((block, rows), lambda j, c: (c[0] * per_half + first + j, 0))
    out = pl.BlockSpec((block, d), lambda j, c: (j, 0))
    n = blocks * block
    extra = [] if got is None else [got]
    return pl.pallas_call(
        functools.partial(dw_kernel, first, block, got is not None, cols // 2),
        grid_spec=pltpu.PrefetchScalarGridSpec(
            num_scalar_prefetch=1,
            grid=(blocks,),
            in_specs=[fixed((rows, d)), fixed((rows, d)), part, part] + [fixed((1, rows))] * 3 + [out] * len(extra),
            out_specs=out,
            scratch_shapes=[pltpu.VMEM((block, rows), BF16)],
        ),
        out_shape=jax.ShapeDtypeStruct((n, d), F32),
        compiler_params=params(),
        cost_estimate=pl.CostEstimate(flops=4 * rows * d * n, bytes_accessed=rows * n * 6 + n * d * 4 * (1 + len(extra)) + rows * d * 4, transcendentals=rows * n),
        name="dw",
    )(which, y0, y1, g0t, z1t, lse, weight, lab, *extra)


def dw_final_kernel(first, block, half_rows, n_in, core_ref, y0_ref, y1_ref, g0_ref, z1_ref, lse_ref, wt_ref, lab_ref, *refs):
    got_ref, fin_ref, big_ref, g1 = refs[0], refs[n_in], refs[n_in + 1], refs[n_in + 2]
    base = core_ref[0] * half_rows + (first + pl.program_id(0)) * block
    v = lax.broadcasted_iota(jnp.int32, z1_ref.shape, 0)
    g1[...] = grad_of(z1_ref[...], lse_ref[...], wt_ref[...], v == lab_ref[...] - base)
    acc = jnp.dot(g0_ref[...], y0_ref[...], preferred_element_type=F32)
    acc += got_ref[...]
    acc += jnp.dot(g1[...], y1_ref[...], preferred_element_type=F32)
    fin_ref[...] = acc
    big_ref[...] = acc


def dw_final(which, y0, y1, g0t, z1t, lse, weight, lab, first, blocks, got, big=None, block=400):
    rows, d = y0.shape
    cols = g0t.shape[0]
    per_half = cols // 2 // block
    fixed = lambda shape: once(shape, lambda j, c: (0, 0))
    part = lambda width: pl.BlockSpec((block, width), lambda j, c: (c[0] * per_half + first + j, 0))
    out = pl.BlockSpec((block, d), lambda j, c: (j, 0))
    n = blocks * block
    extra = [] if big is None else [big]
    n_in = 1 + len(extra)
    return pl.pallas_call(
        functools.partial(dw_final_kernel, first, block, cols // 2, n_in),
        grid_spec=pltpu.PrefetchScalarGridSpec(
            num_scalar_prefetch=1,
            grid=(blocks,),
            in_specs=[fixed((rows, d)), fixed((rows, d)), part(rows), part(rows)] + [fixed((1, rows))] * 3 + [out] + [pl.BlockSpec(memory_space=pl.ANY)] * len(extra),
            out_specs=[out, part(d)],
            scratch_shapes=[pltpu.VMEM((block, rows), BF16)],
        ),
        out_shape=[jax.ShapeDtypeStruct((n, d), F32), jax.ShapeDtypeStruct((cols, d), F32)],
        input_output_aliases={9: 1} if extra else {},
        compiler_params=params(),
        cost_estimate=pl.CostEstimate(flops=4 * rows * d * n, bytes_accessed=rows * n * 6 + n * d * 12 + rows * d * 4, transcendentals=rows * n),
        name="dw_final",
    )(which, y0, y1, g0t, z1t, lse, weight, lab, got, *extra)


def place_kernel(which_ref, src_ref, big_in, big_ref):
    big_ref[...] = src_ref[...]


def place(which, src, big, first, block=400):
    n, d = src.shape
    cols = big.shape[0]
    per_half = cols // 2 // block
    return pl.pallas_call(
        place_kernel,
        grid_spec=pltpu.PrefetchScalarGridSpec(
            num_scalar_prefetch=1,
            grid=(n // block,),
            in_specs=[pl.BlockSpec((block, d), lambda j, c: (j, 0)), pl.BlockSpec(memory_space=pl.ANY)],
            out_specs=pl.BlockSpec((block, d), lambda j, c: (c[0] * per_half + first + j, 0)),
        ),
        out_shape=jax.ShapeDtypeStruct(big.shape, F32),
        input_output_aliases={2: 0},
        compiler_params=params(),
        cost_estimate=pl.CostEstimate(flops=n * d * 100, bytes_accessed=n * d * 8, transcendentals=0),
        name="place",
    )(which, src, big)


def tail_kernel(dy_ref, h_ref, gain_ref, dh_ref, dg_ref):
    @pl.when(pl.program_id(0) == 0)
    def _():
        dg_ref[...] = jnp.zeros(dg_ref.shape, F32)

    x = h_ref[...].astype(F32)
    r = lax.rsqrt(jnp.mean(x * x, axis=-1, keepdims=True) + NORM_EPS)
    x = x * r
    dy = dy_ref[...]
    u = dy * gain_ref[...]
    dh_ref[...] = (r * (u - x * jnp.mean(u * x, axis=-1, keepdims=True))).astype(BF16)
    n, d = x.shape
    dg_ref[...] += jnp.sum((dy * x).reshape(n // 8, 8, d), axis=0)


def tail(dy, hidden, gain, block=256):
    rows, d = dy.shape
    row = lambda: pl.BlockSpec((block, d), lambda i: (i, 0))
    return pl.pallas_call(
        tail_kernel,
        grid=(rows // block,),
        in_specs=[row(), row(), once((1, d), lambda i: (0, 0))],
        out_specs=[row(), once((8, d), lambda i: (0, 0))],
        out_shape=[jax.ShapeDtypeStruct((rows, d), BF16), jax.ShapeDtypeStruct((8, d), F32)],
        compiler_params=params(),
        cost_estimate=pl.CostEstimate(flops=rows * d * 100, bytes_accessed=rows * d * 8, transcendentals=rows),
        name="tail",
    )(dy, hidden, gain)


def solution(mesh):
    n_tp = mesh.shape["tp"]
    n_dp = mesh.shape["dp"]
    half = n_dp // 2
    swap_x = [(i, (i + half) % n_dp) for i in range(n_dp)]
    swap_core = [(i, i ^ 1) for i in range(n_dp)]
    barrier = lax.optimization_barrier

    def dp_sum(v):
        total = v
        for k in range(1, n_dp):
            total = total + lax.ppermute(v, "dp", [(i, i ^ k) for i in range(n_dp)])
        return total

    def local_head(hidden, labels, loss_mask, norm_gain, w_out):
        return body(hidden, labels, loss_mask, norm_gain, w_out.T)

    def body(hidden, labels, loss_mask, norm_gain, wt):
        rows, d = hidden.shape
        cols = wt.shape[0]
        tp = lax.axis_index("tp")
        core = (lax.axis_index("dp") % 2).astype(jnp.int32)
        own_id = core.reshape(1)
        other_id = 1 - own_id
        start = tp * cols

        mask_f = loss_mask.astype(F32)
        gain_f = norm_gain.astype(F32)

        def normed(h):
            h = h.astype(F32)
            return h * lax.rsqrt(jnp.mean(h * h, axis=-1, keepdims=True) + NORM_EPS)

        direct = rows // 4
        quarter = (rows - direct) // n_tp
        mine = normed(lax.dynamic_slice_in_dim(hidden, direct + tp * quarter, quarter, 0))
        straight = normed(hidden[:direct])
        count = jnp.full((8, 128), jnp.sum(mask_f))
        small = jnp.stack([labels, loss_mask])
        mine, straight, small, count, hidden = barrier((mine, straight, small, count, hidden))
        far_q = lax.ppermute(mine, "dp", swap_x)
        far_s = lax.ppermute(straight, "dp", swap_x)
        small_far = lax.ppermute(small, "dp", swap_x)
        mask_total = dp_sum(count)[0, 0]
        far_g = lax.all_gather(far_q, "tp", axis=0, tiled=True)
        y0 = barrier((normed(hidden) * gain_f).astype(BF16))

        def merge(m8, s8, t8):
            m = jnp.max(m8, axis=0)
            s = jnp.sum(s8 * jnp.exp(m8 - m), axis=0)
            stats = [m, s] if t8 is None else [m, s, jnp.sum(t8, axis=0)]
            stats = lax.all_gather(jnp.stack(stats), "tp")
            m_all = jnp.max(stats[:, 0], axis=0)
            s_all = jnp.sum(stats[:, 1] * jnp.exp(stats[:, 0] - m_all), axis=0)
            return m_all + jnp.log(s_all), None if t8 is None else jnp.sum(stats[:, 2], axis=0)

        lab0 = (labels - start)[None]
        z0, m8, s8, t8 = logits(y0, wt, lab0, nt=True)
        lse0, t0 = merge(m8, s8, t8)
        w0 = mask_f / mask_total
        g0, dy = grad_and_dy(z0, wt, lse0[None], w0[None], lab0, chunk=1024)
        d_normed = lax.psum(dy, "tp")

        far_s, far_g, small_far, gain_1, g0, _ = barrier((far_s, far_g, small_far, gain_f, g0, dy))
        y1 = (jnp.concatenate([far_s, far_g], 0) * gain_1).astype(BF16)
        z1, m8, s8 = logits(y1, wt, None, nt=True)
        lse1, _ = merge(m8, s8, None)
        lab1 = (small_far[0] - start)[None]
        w1 = small_far[1].astype(F32) / mask_total
        args = (y0, y1, g0, z1, lse1[None], w1[None], lab1)
        n = cols // 800 // 2
        pa = dw_part(other_id, *args, 0, n)
        got_a = lax.ppermute(pa, "dp", swap_core)
        pb = dw_part(other_id, *args, n, n)
        got_b = lax.ppermute(pb, "dp", swap_core)
        got_a, pb = barrier((got_a, pb))
        fa, big = dw_final(own_id, *args, 0, n, got_a)
        peer_a = lax.ppermute(fa, "dp", swap_core)
        fb, big = dw_final(own_id, *args, n, n, got_b, big)
        peer_b = lax.ppermute(fb, "dp", swap_core)
        big = place(other_id, peer_a, big, 0)
        d_normed, big = barrier((d_normed, big))
        d_hidden, dg8 = tail(d_normed, hidden, gain_f[None])
        big = place(other_id, peer_b, big, n)

        loss_part = jnp.sum(w0 * (lse0 - t0))
        sums = lax.psum(jnp.concatenate([jnp.sum(dg8, axis=0), jnp.full((128,), loss_part)]), "dp")
        return sums[d], d_hidden, big.T, sums[:d]

    return jax.shard_map(local_head, mesh=mesh, in_specs=(P("dp", None), P("dp"), P("dp"), P(), P(None, "tp")), out_specs=(P(), P("dp", None), P(None, "tp"), P()), check_vma=False)
```
